1024 devices in a mesh: dp: 64 (over x, z), tensor: 16 (over y, core).
Axes of the slice: x: 4, y: 8, z: 16, core: 2. Of those that a mesh axis runs over, the one named last changes fastest.
Arguments:
- logits: bfloat16 [128, 128, 77824], P('dp', None, 'tensor'), may hold values from -110 to 290
- token_ids: int32 [128, 128], P('dp'), may hold values from 0 to 77823
- response_mask: int32 [128, 128], P('dp'), may hold values 0 or 1
- lengths: int32 [128], P('dp'), may hold values from 16 to 128
- prompt_of: int32 [128], P('dp'), may hold values from 0 to 15, as said below
- old_logprob: float32 [128, 128], P('dp'), may hold values from -14 to -10
- ref_logprob: bfloat16 [128, 128], P(None, 'dp'), may hold values from -14 to -10
- advantages: float32 [128, 128], P('dp'), may hold values from -8 to 8
- returns: float32 [128, 128], P('dp'), may hold values from -6 to 6
- critic_hidden: bfloat16 [128, 128, 5120], P(None, 'dp', 'tensor'), may hold values from -6 to 6
- value_weight: bfloat16 [5120], P('tensor'), may hold values from -0.078125 to 0.078125
Outputs:
- token_loss: float32 [128, 128], P('dp')
- critic_grad: bfloat16 [128, 128, 5120], P(None, 'dp', 'tensor')
The draws below stay inside these ranges and needn't reach their ends.
Inputs may be any that keep to these rules, and one draw needn't show every extreme that they name: `prompt_of`: each of the 16 prompts is named by exactly 8 sequences.
All inputs are finite; a program needn't handle non-finite values. No bound on the sum of `response_mask` on one device may be relied on, other than what follows from the above.
Results may differ from the reference program's by a relative error of at most 0.001.
Values may be sent and summed in bfloat16 or wider, within the bound.
A program may use at most 32 MiB of HBM per device.

```python
import math
import jax
import jax.numpy as jnp
import numpy as np
from jax import lax

D = 5120
LEN = 128
RESPONSES = 8
BATCH = 128
VOCAB = 77824
PROMPTS = 16


def draw_logits(key, part):
    first_key = jax.random.fold_in(key, 0)
    full_shape = (BATCH, LEN, VOCAB)
    values = 1.5 * jax.random.truncated_normal(first_key, -6.0, 6.0, full_shape, jnp.float32)
    return values.astype(jnp.bfloat16)


def draw_prompt_of(key, part):
    order = jax.random.permutation(jax.random.fold_in(key, 7), BATCH)
    return (order // RESPONSES).astype(jnp.int32)


def touch_ends(result, rng, least, high):
    longest = result.shape.index(max(result.shape))
    spots = []
    for shift in (0, 1):
        where = [jax.random.randint(jax.random.fold_in(rng, axis), (), 0, length) for axis, length in enumerate(result.shape)]
        where[longest] = (where[longest] + shift) % result.shape[longest]
        spots.append(tuple(where))
    return result.at[spots[0]].set(least).at[spots[1]].set(high)


def block_scale(stream_key, shape, cuts, low, top_value):
    factor_of, own = 1.0, jax.random.fold_in(stream_key, 6)
    for dim, parts in cuts:
        steps = jnp.exp(jax.random.uniform(jax.random.fold_in(own, dim), (parts,), jnp.float32, low / len(cuts), top_value / len(cuts)))
        factor_of = factor_of * jnp.repeat(steps, shape[dim] // parts).reshape([-1 if axis == dim else 1 for axis in range(len(shape))])
    return factor_of


def ranked_wide(own_key, dims, amount, slope):
    loads = [min(1 << octave, amount + 1 - (1 << octave)) * (1 << 20) // math.isqrt((1 << octave) ** slope) + 1 for octave in range((amount + 1).bit_length()) if 1 << octave <= amount]
    scale = 1 + sum(loads) // (1 << 30)
    table = np.cumsum(np.array([max(1, weight // scale) for weight in loads]))
    pick = jax.random.randint(jax.random.fold_in(own_key, 1), dims, 0, int(table[len(loads) - 1]))
    start = jnp.left_shift(1, jnp.searchsorted(jnp.asarray(table, jnp.int32), pick, side="right").astype(jnp.int32))
    rank = start - 1 + jax.random.randint(jax.random.fold_in(own_key, 4), dims, 0, 1 << 30) % jnp.minimum(start, amount + 1 - start)
    return jax.random.permutation(jax.random.fold_in(own_key, 2), amount)[rank].astype(jnp.int32)


def normal_values(key, dims, deviation, limit, cuts=(), kind=jnp.bfloat16):
    array = deviation * jax.random.normal(key, dims, jnp.float32)
    if cuts:
        array = array * block_scale(key, dims, cuts, -0.22, 0.18)
    return jnp.clip(array, -limit, limit).astype(kind)


def setup_inputs(seed: int = 0) -> dict:
    keys = jax.random.split(jax.random.key(seed), 12)
    return {
        "logits": draw_logits(jax.random.fold_in(keys[11], 71), 0),
        "token_ids": touch_ends(ranked_wide(keys[1], (BATCH, LEN), VOCAB, 2), jax.random.fold_in(keys[1], 3), 0, VOCAB - 1).astype(jnp.int32),
        "response_mask": touch_ends((jax.random.randint(keys[2], (BATCH, LEN), 0, 8) < 7).astype(jnp.int32), jax.random.fold_in(keys[2], 1), 0, 1),
        "lengths": touch_ends(jax.random.randint(keys[3], (BATCH,), LEN // 8, LEN + 1), jax.random.fold_in(keys[3], 1), LEN // 8, LEN).astype(jnp.int32),
        "prompt_of": draw_prompt_of(jax.random.fold_in(keys[11], 71), 0),
        "old_logprob": jnp.clip(-14.0 + 4.0 * jax.random.uniform(keys[5], (BATCH, LEN), jnp.float32) ** block_scale(keys[5], (BATCH, LEN), ((0, 64),), -0.2, 0.2), -14.0, -10.0),
        "ref_logprob": jnp.clip(-14.0 + 4.0 * jax.random.uniform(keys[6], (BATCH, LEN), jnp.float32) ** block_scale(keys[6], (BATCH, LEN), ((1, 64),), -0.2, 0.2), -14.0, -10.0).astype(jnp.bfloat16),
        "advantages": normal_values(keys[7], (BATCH, LEN), 2.0, 8.0, ((0, 64),), jnp.float32),
        "returns": normal_values(keys[8], (BATCH, LEN), 1.0, 6.0, ((0, 64),), jnp.float32),
        "critic_hidden": normal_values(keys[9], (BATCH, LEN, D), 1.0, 6.0, ((1, 64), (2, 16))),
        "value_weight": normal_values(keys[10], (D,), D ** -0.5, 0.078125, ((0, 16),)),
    }


def token_logprob(inputs):
    row_block, row_ids = inputs
    row_max = lax.optimization_barrier(jnp.max(row_block, axis=1)).astype(jnp.float32)
    exp_total = lax.optimization_barrier(jnp.sum(jnp.exp(row_block.astype(jnp.float32) - row_max[:, None]), axis=1))
    picked = jnp.take_along_axis(row_block, row_ids[:, None].astype(jnp.int32), axis=1)[:, 0].astype(jnp.float32)
    return picked - (row_max + jnp.log(exp_total))

def reference(logits, token_ids, response_mask, lengths, prompt_of, old_logprob, ref_logprob, advantages, returns, critic_hidden, value_weight):
    highest = lax.Precision.HIGHEST
    logprob = lax.map(token_logprob, (logits, token_ids))
    head_weight = value_weight.astype(jnp.float32)
    value_pred = jnp.einsum('bld,d->bl', critic_hidden.astype(jnp.float32), head_weight)
    position = jnp.arange(LEN, dtype=jnp.int32)
    live_mask = (response_mask * (position[None, :] < lengths[:, None]).astype(jnp.int32)).astype(jnp.float32)
    prompt_hot = (prompt_of[:, None] == jnp.arange(PROMPTS, dtype=jnp.int32)[None, :]).astype(jnp.float32)
    seq_tokens = lax.optimization_barrier(jnp.sum(live_mask, axis=1))
    seq_total = lax.optimization_barrier(jnp.sum(live_mask * advantages, axis=1))
    count_floor = jnp.maximum(jnp.dot(seq_tokens, prompt_hot, precision=highest), 1.0)
    prompt_mean = jnp.dot(seq_total, prompt_hot, precision=highest) / count_floor
    row_mean = jnp.dot(prompt_hot, prompt_mean, precision=highest)
    centered = advantages - row_mean[:, None]
    seq_square = lax.optimization_barrier(jnp.sum(live_mask * centered * centered, axis=1))
    prompt_var = jnp.dot(seq_square, prompt_hot, precision=highest) / count_floor
    row_scale = 1.0 / jnp.sqrt(jnp.dot(prompt_hot, prompt_var, precision=highest) + 1.0)
    whitened = centered * row_scale[:, None]
    prob_ratio = jnp.exp(jnp.clip(logprob - old_logprob, -20.0, 20.0))
    surrogate = jnp.maximum(-whitened * prob_ratio, -whitened * jnp.clip(prob_ratio, 0.8, 1.2))
    surrogate = jnp.where(whitened < 0.0, jnp.minimum(surrogate, -3.0 * whitened), surrogate)
    ref_drift = jnp.clip(ref_logprob.astype(jnp.float32) - logprob, -20.0, 20.0)
    penalty = jnp.clip(jnp.exp(ref_drift) - ref_drift - 1.0, -10.0, 10.0)
    value_error = value_pred - returns
    token_loss = live_mask * (surrogate + 0.1 * penalty + 0.25 * value_error * value_error)
    grad_coeff = 32.0 * live_mask * value_error
    critic_grad = (grad_coeff[:, :, None] * head_weight[None, None, :]).astype(jnp.bfloat16)
    return (token_loss, critic_grad)
```

```python
import functools

import jax
import jax.numpy as jnp
from jax import lax
from jax.experimental import pallas as pl
from jax.experimental.pallas import tpu as pltpu
from jax.sharding import PartitionSpec as P

MESH = pl.DeviceIdType.MESH
F32 = jnp.float32
DEAD = 1e30
BLOCK = 16


def far_first(k, half):
    back = lax.rem(k, 2)
    return half + (1 - back) * (k // 2) - back * ((k + 1) // 2)


def kernel(
    xs, zs, ys, vocab,
    logits, ids, mask, lengths, prompt_of, old, ref_t, adv, ret, critic, weight,
    loss_out, grad_out,
    lg, cr, ids_v, mask_v, old_v, ref_v, adv_v, ret_v, w_v, grad_v,
    stage, msg, inbox, quiet, idt, stt, t1_src, t1, t2_src, t2,
    lg_sem, in_sem, out_sem, dp_send, dp_recv, t1_send, t1_recv, t2_send, t2_recv,
):
    dp, tp = lax.axis_index("dp"), lax.axis_index("tensor")
    n_dp, n_tp = xs * zs, 2 * ys
    my_x, my_z, my_y, my_c = dp // zs, lax.rem(dp, zs), tp // 2, lax.rem(tp, 2)

    def dp_peer(i):
        dz, dx = far_first(i // xs, zs // 2), lax.rem(lax.rem(i, xs) + 1, xs)
        return lax.rem(my_x + dx, xs) * zs + lax.rem(my_z + dz, zs)

    def tp_peer(i):
        dy, dc = far_first(i // 2, ys // 2), lax.rem(lax.rem(i, 2) + 1, 2)
        return lax.rem(my_y + dy, ys) * 2 + lax.rem(my_c + dc, 2)

    smalls = [
        pltpu.make_async_copy(src, dst, in_sem.at[n])
        for n, (src, dst) in enumerate(
            [
                (critic, cr), (weight, w_v), (ref_t, ref_v), (mask, mask_v), (adv, adv_v),
                (ret, ret_v), (ids, ids_v), (old, old_v),
            ]
        )
    ]
    for copy in smalls:
        copy.start()
    barrier = pltpu.get_barrier_semaphore()

    def greet_dp(i, carry):
        pl.semaphore_signal(barrier, inc=1, device_id={"dp": dp_peer(i)}, device_id_type=MESH)
        return carry

    def greet_tp(i, carry):
        pl.semaphore_signal(barrier, inc=1, device_id={"tensor": tp_peer(i)}, device_id_type=MESH)
        return carry

    lax.fori_loop(0, n_dp - 1, greet_dp, 0)
    lax.fori_loop(0, n_tp - 1, greet_tp, 0)
    chunks = []
    for b in range(2):
        for h in range(2):
            rows = pl.ds(h * 64, 64)
            chunks.append(
                pltpu.make_async_copy(logits.at[b, rows], lg.at[b, rows], lg_sem.at[b * 2 + h])
            )
            chunks[-1].start()
    for copy in smalls:
        copy.wait()

    row2 = lax.broadcasted_iota(jnp.int32, (2, 128), 0)
    lane2 = lax.broadcasted_iota(jnp.int32, (2, 128), 1)
    length_of = jnp.where(row2 == 0, lengths[0], lengths[1])
    live = (mask_v[...] * (lane2 < length_of).astype(jnp.int32)).astype(F32)
    advantages, returns = adv_v[...], ret_v[...]
    live_adv = live * advantages

    def spread(column):
        return jnp.broadcast_to(jnp.sum(column, axis=1, keepdims=True), (2, 128))

    feats = w_v.shape[1]
    w_row = jnp.pad(w_v[...].astype(F32), ((0, 0), (0, -feats % 128)))
    w_all = jnp.transpose(jnp.broadcast_to(w_row, (128, w_row.shape[1])))[:feats]
    parts = [
        jnp.sum(cr[j].astype(F32) * w_all, axis=0, keepdims=True) for j in range(2)
    ]
    pid = jnp.where(row2 == 0, prompt_of[0], prompt_of[1]).astype(F32)
    lines = jnp.concatenate(
        parts
        + [
            ref_v[...].astype(F32),
            jnp.where(live > 0.0, returns, DEAD),
            spread(live),
            spread(live_adv),
            spread(live_adv * advantages),
            pid,
            jnp.zeros((114, 128), F32),
        ],
        axis=0,
    )
    stage[...] = jnp.transpose(lines)
    packed = stage[pl.ds(0, 64, stride=2), :] + pltpu.roll(stage[pl.ds(1, 64, stride=2), :], 16, 1)
    msg[...] = packed[:, None, :]
    inbox[pl.ds(dp, 1)] = msg[pl.ds(dp, 1)]

    pl.semaphore_wait(barrier, n_dp - 1 + n_tp - 1)

    def send_dp(i, carry):
        peer = dp_peer(i)
        pltpu.make_async_remote_copy(
            src_ref=msg.at[peer],
            dst_ref=inbox.at[dp],
            send_sem=dp_send,
            recv_sem=dp_recv,
            device_id={"dp": peer},
            device_id_type=MESH,
        ).start()
        return carry

    lax.fori_loop(0, n_dp - 1, send_dp, 0)

    shifted = jnp.pad((ids_v[...] - tp * vocab).astype(F32), ((0, 6), (0, 0)))
    idt[...] = jnp.transpose(shifted).astype(jnp.int32)
    stt[...] = jnp.zeros((128, 128), F32)
    lane = lax.broadcasted_iota(jnp.int32, (BLOCK, 128), 1)
    for b in range(2):
        for h in range(2):
            chunks[b * 2 + h].wait()

            def token_block(i, carry):
                rows = pl.ds(pl.multiple_of(h * 64 + i * BLOCK, BLOCK), BLOCK)
                top = lg[b, rows, pl.ds(0, 128)]
                for c in range(1, vocab // 128):
                    top = jnp.maximum(top, lg[b, rows, pl.ds(c * 128, 128)])
                top = jnp.max(top.astype(F32), axis=1, keepdims=True)
                tops = jnp.broadcast_to(top, (BLOCK, 128))
                wanted = jnp.broadcast_to(idt[rows, b : b + 1], (BLOCK, 128))
                total = jnp.zeros((BLOCK, 128), F32)
                found = jnp.zeros((BLOCK, 128), F32)
                for c in range(vocab // 128):
                    x = lg[b, rows, pl.ds(c * 128, 128)].astype(F32)
                    total = total + jnp.exp(x - tops)
                    found = jnp.where(wanted == lane + c * 128, x, found)
                stt[rows, b : b + 1] = top
                stt[rows, 2 + b : 3 + b] = jnp.sum(total, axis=1, keepdims=True)
                stt[rows, 4 + b : 5 + b] = jnp.sum(found, axis=1, keepdims=True)
                return carry

            lax.fori_loop(0, 64 // BLOCK, token_block, 0)
    t1_src[0:6] = jnp.transpose(stt[...])[0:6]
    t1_src[6:8] = jnp.concatenate(parts, axis=0)
    t1[pl.ds(tp, 1)] = t1_src[...][None]

    def send_t1(i, carry):
        pltpu.make_async_remote_copy(
            src_ref=t1_src,
            dst_ref=t1.at[tp],
            send_sem=t1_send,
            recv_sem=t1_recv,
            device_id={"tensor": tp_peer(i)},
            device_id_type=MESH,
        ).start()
        return carry

    lax.fori_loop(0, n_tp - 1, send_t1, 0)

    def all_but_one(ref, sem):
        some = ref.at[pl.ds(0, ref.shape[0] - 1)]
        return pltpu.make_async_copy(some, some, sem)

    all_but_one(inbox, dp_recv).wait()
    got = inbox[...][:, 0, :]
    quiet[pl.ds(0, 64, stride=2), :] = got
    quiet[pl.ds(1, 64, stride=2), :] = pltpu.roll(got, 127, 1)
    turned = jnp.transpose(quiet[...])

    def pair(k):
        return jnp.concatenate([turned[k : k + 1], turned[16 + k : 17 + k]], axis=0)

    t2_src[...] = pair(0)
    t2[pl.ds(tp, 1)] = t2_src[...][None]

    def send_t2(i, carry):
        pltpu.make_async_remote_copy(
            src_ref=t2_src,
            dst_ref=t2.at[tp],
            send_sem=t2_send,
            recv_sem=t2_recv,
            device_id={"tensor": tp_peer(i)},
            device_id_type=MESH,
        ).start()
        return carry

    lax.fori_loop(0, n_tp - 1, send_t2, 0)

    ref_rows, held_returns = pair(2), pair(4)
    same = (turned[12:13] == pid).astype(F32)
    count = jnp.sum(same * turned[6:7], axis=1, keepdims=True)
    summed = jnp.sum(same * turned[8:9], axis=1, keepdims=True)
    square = jnp.sum(same * turned[10:11], axis=1, keepdims=True)
    floor = jnp.maximum(count, 1.0)
    mean = summed / floor
    var = (square - mean * summed) / floor
    whitened = (advantages - mean) * lax.rsqrt(var + 1.0)

    all_but_one(t1, t1_recv).wait()
    shards = t1[...]
    values = jnp.sum(shards[:, 6:8], axis=0)
    coeff = jnp.where(held_returns > 1e29, 0.0, 32.0 * (values - held_returns))
    for j in range(2):
        grad_v[j] = (w_all * coeff[j : j + 1]).astype(jnp.bfloat16)
    grad_copy = pltpu.make_async_copy(grad_v, grad_out, out_sem)
    grad_copy.start()

    tops = shards[:, 0:2]
    row_max = jnp.max(tops, axis=0)
    total = jnp.sum(shards[:, 2:4] * jnp.exp(tops - row_max[None]), axis=0)
    target = jnp.sum(shards[:, 4:6], axis=0)
    logprob = target - (row_max + jnp.log(total))
    ratio = jnp.exp(jnp.clip(logprob - old_v[...], -20.0, 20.0))
    surrogate = jnp.maximum(-whitened * ratio, -whitened * jnp.clip(ratio, 0.8, 1.2))
    surrogate = jnp.where(whitened < 0.0, jnp.minimum(surrogate, -3.0 * whitened), surrogate)
    drift = jnp.clip(ref_rows - logprob, -20.0, 20.0)
    penalty = jnp.clip(jnp.exp(drift) - drift - 1.0, -10.0, 10.0)
    policy = surrogate + 0.1 * penalty

    all_but_one(t2, t2_recv).wait()
    error = jnp.sum(t2[...], axis=0) - returns
    loss_out[...] = live * (policy + 0.25 * error * error)

    all_but_one(inbox, dp_send).wait()
    all_but_one(t1, t1_send).wait()
    all_but_one(t2, t2_send).wait()
    grad_copy.wait()


def per_device(sizes, *arrays):
    (
        logits, ids, mask, lengths, prompt_of, old, ref, adv, ret, critic, weight
    ) = arrays
    seqs, length, vocab = logits.shape
    batch, tile, feats = critic.shape
    xs, zs, ys = sizes
    any_ref, smem = pl.BlockSpec(memory_space=pl.ANY), pl.BlockSpec(memory_space=pltpu.SMEM)
    dma = pltpu.SemaphoreType.DMA
    vm = pltpu.VMEM
    loss, grad = pl.pallas_call(
        functools.partial(kernel, xs, zs, ys, vocab),
        out_shape=(
            jax.ShapeDtypeStruct((seqs, length), F32),
            jax.ShapeDtypeStruct((tile, feats, batch), jnp.bfloat16),
        ),
        in_specs=[any_ref] * 3 + [smem] * 2 + [any_ref] * 6,
        out_specs=(pl.BlockSpec(memory_space=pltpu.VMEM), any_ref),
        scratch_shapes=[
            vm(logits.shape, jnp.bfloat16),
            vm((tile, feats, batch), jnp.bfloat16),
            vm((seqs, length), jnp.int32),
            vm((seqs, length), jnp.int32),
            vm((seqs, length), F32),
            vm((tile, batch), jnp.bfloat16),
            vm((seqs, length), F32),
            vm((seqs, length), F32),
            vm((1, feats), jnp.bfloat16),
            vm((tile, feats, batch), jnp.bfloat16),
            vm((128, 128), F32),
            vm((64, 1, 128), F32),
            vm((64, 1, 128), F32),
            vm((128, 128), F32),
            vm((128, 8), jnp.int32),
            vm((128, 128), F32),
            vm((8, 128), F32),
            vm((2 * ys, 8, 128), F32),
            vm((seqs, length), F32),
            vm((2 * ys, seqs, length), F32),
            dma((4,)), dma((8,)), dma, dma, dma, dma, dma, dma, dma,
        ],
        compiler_params=pltpu.CompilerParams(collective_id=0, has_side_effects=True),
        name="ppo_all",
    )(
        logits, ids, mask, lengths, prompt_of, old, ref.T, adv, ret,
        jnp.transpose(critic, (1, 2, 0)), weight.reshape(1, feats),
    )
    return loss, jnp.transpose(grad, (2, 0, 1))


def solution(mesh):
    in_specs = (
        P("dp", None, "tensor"),
        P("dp", None),
        P("dp", None),
        P("dp"),
        P("dp"),
        P("dp", None),
        P(None, "dp"),
        P("dp", None),
        P("dp", None),
        P(None, "dp", "tensor"),
        P("tensor"),
    )
    out_specs = (P("dp", None), P(None, "dp", "tensor"))
    dp_size, tp_size = mesh.shape["dp"], mesh.shape["tensor"]
    sizes = (4, dp_size // 4, tp_size // 2)
    return jax.shard_map(
        functools.partial(per_device, sizes),
        mesh=mesh,
        in_specs=in_specs,
        out_specs=out_specs,
        check_vma=False,
    )
```

```python
import functools
import itertools

import jax
import jax.numpy as jnp
from jax import lax
from jax.experimental import pallas as pl
from jax.experimental.pallas import tpu as pltpu
from jax.sharding import PartitionSpec as P

MESH = pl.DeviceIdType.MESH
F32 = jnp.float32
DEAD = 1e30
BLOCK = 16


def far_first(*sizes):
    offsets = itertools.product(*(range(n) for n in sizes))
    return sorted(offsets, key=lambda o: -sum(min(d, n - d) for d, n in zip(o, sizes)))[:-1]


def kernel(
    xs, zs, ys, vocab,
    logits, ids, mask, lengths_in, prompt_in, old, ref_t, adv, ret, critic, weight,
    loss_out, grad_out,
    lg, cr, ids_v, mask_v, old_v, ref_v, adv_v, ret_v, w_v, lengths, prompt_of,
    stage, msg, inbox, quiet, idt, stt, t1_src, t1, t2_src, t2,
    lg_sem, in_sem, dp_send, dp_recv, t1_send, t1_recv, t2_send, t2_recv,
):
    dp, tp = lax.axis_index("dp"), lax.axis_index("tensor")
    n_dp, n_tp = xs * zs, 2 * ys
    my_x, my_z, my_y, my_c = dp // zs, lax.rem(dp, zs), tp // 2, lax.rem(tp, 2)

    smalls = [
        pltpu.make_async_copy(src, dst, in_sem.at[n])
        for n, (src, dst) in enumerate(
            [
                (critic, cr), (weight, w_v), (ref_t, ref_v), (mask, mask_v), (adv, adv_v),
                (lengths_in, lengths), (prompt_in, prompt_of), (ret, ret_v), (ids, ids_v), (old, old_v),
            ]
        )
    ]
    for copy in smalls:
        copy.start()
    at_x = [lax.rem(my_x + d, xs) * zs for d in range(xs)]
    at_z = [lax.rem(my_z + d, zs) for d in range(zs)]
    at_y = [lax.rem(my_y + d, ys) * 2 for d in range(ys)]
    at_c = [my_c, 1 - my_c]
    dp_peers = [at_x[x] + at_z[z] for x, z in far_first(xs, zs)]
    tp_peers = [at_y[y] + at_c[c] for y, c in far_first(ys, 2)]

    barrier = pltpu.get_barrier_semaphore()

    for peer in dp_peers:
        pl.semaphore_signal(barrier, inc=1, device_id={"dp": peer}, device_id_type=MESH)
    for peer in tp_peers:
        pl.semaphore_signal(barrier, inc=1, device_id={"tensor": peer}, device_id_type=MESH)
    chunks = []
    for b in range(2):
        for h in range(2):
            rows = pl.ds(h * 64, 64)
            chunks.append(
                pltpu.make_async_copy(logits.at[b, rows], lg.at[b, rows], lg_sem.at[b * 2 + h])
            )
            chunks[-1].start()
    for copy in smalls:
        copy.wait()

    row2 = lax.broadcasted_iota(jnp.int32, (2, 128), 0)
    lane2 = lax.broadcasted_iota(jnp.int32, (2, 128), 1)
    length_of = jnp.where(row2 == 0, lengths[0], lengths[1])
    live = (mask_v[...] * (lane2 < length_of).astype(jnp.int32)).astype(F32)
    advantages, returns = adv_v[...], ret_v[...]
    live_adv = live * advantages

    def spread(column):
        return jnp.broadcast_to(jnp.sum(column, axis=1, keepdims=True), (2, 128))

    feats = w_v.shape[0]
    w_row = jnp.pad(w_v[...].astype(F32).reshape(1, feats), ((0, 0), (0, -feats % 128)))
    w_all = jnp.transpose(jnp.broadcast_to(w_row, (128, w_row.shape[1])))[:feats]
    parts = [
        jnp.sum(cr[j].astype(F32) * w_all, axis=0, keepdims=True) for j in range(2)
    ]
    pid = jnp.where(row2 == 0, prompt_of[0], prompt_of[1]).astype(F32)
    lines = jnp.concatenate(
        parts
        + [
            ref_v[...].astype(F32),
            jnp.where(live > 0.0, returns, DEAD),
            spread(live),
            spread(live_adv),
            spread(live_adv * advantages),
            pid,
            jnp.zeros((114, 128), F32),
        ],
        axis=0,
    )
    stage[...] = jnp.transpose(lines)
    packed = stage[pl.ds(0, 64, stride=2), :] + pltpu.roll(stage[pl.ds(1, 64, stride=2), :], 16, 1)
    msg[...] = packed[:, None, :]
    inbox[pl.ds(dp, 1)] = msg[pl.ds(dp, 1)]

    pl.semaphore_wait(barrier, n_dp - 1 + n_tp - 1)

    for peer in dp_peers:
        pltpu.make_async_remote_copy(
            src_ref=msg.at[peer],
            dst_ref=inbox.at[dp],
            send_sem=dp_send,
            recv_sem=dp_recv,
            device_id={"dp": peer},
            device_id_type=MESH,
        ).start()

    shifted = jnp.pad((ids_v[...] - tp * vocab).astype(F32), ((0, 6), (0, 0)))
    idt[...] = jnp.transpose(shifted).astype(jnp.int32)
    stt[...] = jnp.zeros((128, 128), F32)
    lane = lax.broadcasted_iota(jnp.int32, (BLOCK, 128), 1)
    for b in range(2):
        for h in range(2):
            chunks[b * 2 + h].wait()

            def token_block(i, carry):
                rows = pl.ds(pl.multiple_of(h * 64 + i * BLOCK, BLOCK), BLOCK)
                top = lg[b, rows, pl.ds(0, 128)]
                for c in range(1, vocab // 128):
                    top = jnp.maximum(top, lg[b, rows, pl.ds(c * 128, 128)])
                top = jnp.max(top.astype(F32), axis=1, keepdims=True)
                tops = jnp.broadcast_to(top, (BLOCK, 128))
                wanted = jnp.broadcast_to(idt[rows, b : b + 1], (BLOCK, 128))
                total = jnp.zeros((BLOCK, 128), F32)
                found = jnp.zeros((BLOCK, 128), F32)
                for c in range(vocab // 128):
                    x = lg[b, rows, pl.ds(c * 128, 128)].astype(F32)
                    total = total + jnp.exp(x - tops)
                    found = jnp.where(wanted == lane + c * 128, x, found)
                stt[rows, b : b + 1] = top
                stt[rows, 2 + b : 3 + b] = jnp.sum(total, axis=1, keepdims=True)
                stt[rows, 4 + b : 5 + b] = jnp.sum(found, axis=1, keepdims=True)
                return carry

            lax.fori_loop(0, 64 // BLOCK, token_block, 0)
    t1_src[0:6] = jnp.transpose(stt[...])[0:6]
    t1_src[6:8] = jnp.concatenate(parts, axis=0)
    t1[pl.ds(tp, 1)] = t1_src[...][None]

    for peer in tp_peers:
        pltpu.make_async_remote_copy(
            src_ref=t1_src,
            dst_ref=t1.at[tp],
            send_sem=t1_send,
            recv_sem=t1_recv,
            device_id={"tensor": peer},
            device_id_type=MESH,
        ).start()

    def all_but_one(ref, sem):
        some = ref.at[pl.ds(0, ref.shape[0] - 1)]
        return pltpu.make_async_copy(some, some, sem)

    all_but_one(inbox, dp_recv).wait()
    got = inbox[...][:, 0, :]
    quiet[pl.ds(0, 64, stride=2), :] = got
    quiet[pl.ds(1, 64, stride=2), :] = pltpu.roll(got, 127, 1)
    turned = jnp.transpose(quiet[...])

    def pair(k):
        return jnp.concatenate([turned[k : k + 1], turned[16 + k : 17 + k]], axis=0)

    t2_src[...] = pair(0)
    t2[pl.ds(tp, 1)] = t2_src[...][None]

    for peer in tp_peers:
        pltpu.make_async_remote_copy(
            src_ref=t2_src,
            dst_ref=t2.at[tp],
            send_sem=t2_send,
            recv_sem=t2_recv,
            device_id={"tensor": peer},
            device_id_type=MESH,
        ).start()

    ref_rows, held_returns = pair(2), pair(4)
    same = (turned[12:13] == pid).astype(F32)
    count = jnp.sum(same * turned[6:7], axis=1, keepdims=True)
    summed = jnp.sum(same * turned[8:9], axis=1, keepdims=True)
    square = jnp.sum(same * turned[10:11], axis=1, keepdims=True)
    floor = jnp.maximum(count, 1.0)
    mean = summed / floor
    var = (square - mean * summed) / floor
    whitened = (advantages - mean) * lax.rsqrt(var + 1.0)

    all_but_one(t1, t1_recv).wait()
    shards = t1[...]
    values = jnp.sum(shards[:, 6:8], axis=0)
    coeff = jnp.where(held_returns > 1e29, 0.0, 32.0 * (values - held_returns))
    for j in range(2):
        grad_out[j] = (w_all * coeff[j : j + 1]).astype(jnp.bfloat16)

    tops = shards[:, 0:2]
    row_max = jnp.max(tops, axis=0)
    total = jnp.sum(shards[:, 2:4] * jnp.exp(tops - row_max[None]), axis=0)
    target = jnp.sum(shards[:, 4:6], axis=0)
    logprob = target - (row_max + jnp.log(total))
    ratio = jnp.exp(jnp.clip(logprob - old_v[...], -20.0, 20.0))
    surrogate = jnp.maximum(-whitened * ratio, -whitened * jnp.clip(ratio, 0.8, 1.2))
    surrogate = jnp.where(whitened < 0.0, jnp.minimum(surrogate, -3.0 * whitened), surrogate)
    drift = jnp.clip(ref_rows - logprob, -20.0, 20.0)
    penalty = jnp.clip(jnp.exp(drift) - drift - 1.0, -10.0, 10.0)
    policy = live * (surrogate + 0.1 * penalty)
    scale = 0.25 * live

    all_but_one(t2, t2_recv).wait()
    error = jnp.sum(t2[...], axis=0) - returns
    loss_out[...] = policy + scale * error * error

    all_but_one(inbox, dp_send).wait()
    all_but_one(t1, t1_send).wait()
    all_but_one(t2, t2_send).wait()


def finish(loss, grad, loss_out, grad_out, sems):
    copies = [
        pltpu.make_async_copy(src, dst, sems.at[n])
        for n, (src, dst) in enumerate([(grad, grad_out), (loss, loss_out)])
    ]
    for copy in copies:
        copy.start()
    for copy in copies:
        copy.wait()


def per_device(sizes, *arrays):
    (
        logits, ids, mask, lengths, prompt_of, old, ref, adv, ret, critic, weight
    ) = arrays
    seqs, length, vocab = logits.shape
    batch, tile, feats = critic.shape
    xs, zs, ys = sizes
    any_ref, vmem = pl.BlockSpec(memory_space=pl.ANY), pl.BlockSpec(memory_space=pltpu.VMEM)
    dma = pltpu.SemaphoreType.DMA
    vm = pltpu.VMEM
    loss, grad = pl.pallas_call(
        functools.partial(kernel, xs, zs, ys, vocab),
        out_shape=(
            vm((seqs, length), F32),
            vm((tile, feats, batch), jnp.bfloat16),
        ),
        in_specs=[any_ref] * 11,
        out_specs=[vmem] * 2,
        scratch_shapes=[
            vm(logits.shape, jnp.bfloat16),
            vm((tile, feats, batch), jnp.bfloat16),
            vm((seqs, length), jnp.int32),
            vm((seqs, length), jnp.int32),
            vm((seqs, length), F32),
            vm((tile, batch), jnp.bfloat16),
            vm((seqs, length), F32),
            vm((seqs, length), F32),
            vm((feats,), jnp.bfloat16),
            pltpu.SMEM((seqs,), jnp.int32),
            pltpu.SMEM((seqs,), jnp.int32),
            vm((128, 128), F32),
            vm((64, 1, 128), F32),
            vm((64, 1, 128), F32),
            vm((128, 128), F32),
            vm((128, 8), jnp.int32),
            vm((128, 128), F32),
            vm((8, 128), F32),
            vm((2 * ys, 8, 128), F32),
            vm((seqs, length), F32),
            vm((2 * ys, seqs, length), F32),
            dma((4,)), dma((10,)), dma, dma, dma, dma, dma, dma,
        ],
        compiler_params=pltpu.CompilerParams(collective_id=0, has_side_effects=True),
        name="ppo_all",
    )(
        logits, ids, mask, lengths, prompt_of, old, ref.T, adv, ret,
        jnp.transpose(critic, (1, 2, 0)), weight,
    )
    loss, grad = pl.pallas_call(
        finish,
        out_shape=(
            jax.ShapeDtypeStruct((seqs, length), F32),
            jax.ShapeDtypeStruct((tile, feats, batch), jnp.bfloat16),
        ),
        in_specs=[vmem] * 2,
        out_specs=[any_ref] * 2,
        scratch_shapes=[dma((2,))],
        compiler_params=pltpu.CompilerParams(vmem_limit_bytes=2**20),
        name="ppo_finish",
    )(loss, grad)
    return loss, jnp.transpose(grad, (2, 0, 1))


def solution(mesh):
    in_specs = (
        P("dp", None, "tensor"),
        P("dp", None),
        P("dp", None),
        P("dp"),
        P("dp"),
        P("dp", None),
        P(None, "dp"),
        P("dp", None),
        P("dp", None),
        P(None, "dp", "tensor"),
        P("tensor"),
    )
    out_specs = (P("dp", None), P(None, "dp", "tensor"))
    dp_size, tp_size = mesh.shape["dp"], mesh.shape["tensor"]
    sizes = (4, dp_size // 4, tp_size // 2)
    return jax.shard_map(
        functools.partial(per_device, sizes),
        mesh=mesh,
        in_specs=in_specs,
        out_specs=out_specs,
        check_vma=False,
    )
```

```python
import functools
import itertools

import jax
import jax.numpy as jnp
from jax import lax
from jax.experimental import pallas as pl
from jax.experimental.pallas import tpu as pltpu
from jax.sharding import PartitionSpec as P

MESH = pl.DeviceIdType.MESH
F32 = jnp.float32
DEAD = 1e30
BLOCK = 16


def far_first(*sizes):
    offsets = itertools.product(*(range(n) for n in sizes))
    return sorted(offsets, key=lambda o: -sum(min(d, n - d) for d, n in zip(o, sizes)))[:-1]


def kernel(
    xs, zs, ys, vocab,
    logits, ids, mask, lengths_in, prompt_in, old, ref_t, adv, ret, critic, weight,
    loss_out, grad_out,
    lg, cr, ids_v, mask_v, old_v, ref_v, adv_v, ret_v, w_v, lengths, prompt_of,
    stage, msg, inbox, relay, quiet, idt, stt, t1_src, t1, t2_src, t2,
    lg_sem, in_sem, dp_send, dp_recv, t1_send, t1_recv, t2_send, t2_recv,
    relay_send, relay_recv, entered, line_in,
):
    dp, tp = lax.axis_index("dp"), lax.axis_index("tensor")
    n_dp, n_tp = xs * zs, 2 * ys
    my_x, my_z, my_y, my_c = dp // zs, lax.rem(dp, zs), tp // 2, lax.rem(tp, 2)

    smalls = [
        pltpu.make_async_copy(src, dst, in_sem.at[n])
        for n, (src, dst) in enumerate(
            [
                (critic, cr), (weight, w_v), (ref_t, ref_v), (mask, mask_v), (adv, adv_v),
                (lengths_in, lengths), (prompt_in, prompt_of), (ret, ret_v), (ids, ids_v), (old, old_v),
            ]
        )
    ]
    for copy in smalls:
        copy.start()
    at_x = [lax.rem(my_x + d, xs) * zs for d in range(xs)]
    at_z = [lax.rem(my_z + d, zs) for d in range(zs)]
    at_y = [lax.rem(my_y + d, ys) * 2 for d in range(ys)]
    at_c = [my_c, 1 - my_c]
    dp_peers = [at_x[x] + at_z[z] for x, z in far_first(xs, zs)]
    half = zs // 2
    near, far = my_z < half, my_z >= half
    partner = my_x * zs + (zs - 1 - my_z)
    at_near = [lax.rem(my_z + d, half) for d in range(half)]
    near_peers = [
        (at_x[x] + at_near[z], at_x[x] + (zs - 1 - at_near[z])) for x, z in far_first(xs, half)
    ]
    own_column = (my_x * zs + at_near[0], my_x * zs + (zs - 1 - at_near[0]))

    tp_peers = [at_y[y] + at_c[c] for y, c in far_first(ys, 2)]

    barrier = pltpu.get_barrier_semaphore()

    @pl.when(near)
    def _():
        for peer in dp_peers:
            pl.semaphore_signal(barrier, inc=1, device_id={"dp": peer}, device_id_type=MESH)
        for peer in tp_peers:
            pl.semaphore_signal(barrier, inc=1, device_id={"tensor": peer}, device_id_type=MESH)

    chunks = []
    for b in range(2):
        for h in range(2):
            rows = pl.ds(h * 64, 64)
            chunks.append(
                pltpu.make_async_copy(logits.at[b, rows], lg.at[b, rows], lg_sem.at[b * 2 + h])
            )
            chunks[-1].start()
    for copy in smalls:
        copy.wait()

    row2 = lax.broadcasted_iota(jnp.int32, (2, 128), 0)
    lane2 = lax.broadcasted_iota(jnp.int32, (2, 128), 1)
    length_of = jnp.where(row2 == 0, lengths[0], lengths[1])
    live = (mask_v[...] * (lane2 < length_of).astype(jnp.int32)).astype(F32)
    advantages, returns = adv_v[...], ret_v[...]
    live_adv = live * advantages

    def spread(column):
        return jnp.broadcast_to(jnp.sum(column, axis=1, keepdims=True), (2, 128))

    feats = w_v.shape[0]
    w_row = jnp.pad(w_v[...].astype(F32).reshape(1, feats), ((0, 0), (0, -feats % 128)))
    w_all = jnp.transpose(jnp.broadcast_to(w_row, (128, w_row.shape[1])))[:feats]
    parts = [
        jnp.sum(cr[j].astype(F32) * w_all, axis=0, keepdims=True) for j in range(2)
    ]
    pid = jnp.where(row2 == 0, prompt_of[0], prompt_of[1]).astype(F32)
    lines = jnp.concatenate(
        parts
        + [
            ref_v[...].astype(F32),
            jnp.where(live > 0.0, returns, DEAD),
            spread(live),
            spread(live_adv),
            spread(live_adv * advantages),
            pid,
            jnp.zeros((114, 128), F32),
        ],
        axis=0,
    )
    stage[...] = jnp.transpose(lines)
    packed = stage[pl.ds(0, 64, stride=2), :] + pltpu.roll(stage[pl.ds(1, 64, stride=2), :], 16, 1)
    msg[...] = packed[:, None, :]

    @pl.when(near)
    def _():
        inbox[pl.ds(dp, 1)] = msg[pl.ds(dp, 1)]
        relay[pl.ds(dp, 1)] = msg[pl.ds(partner, 1)]

    pl.semaphore_wait(barrier, jnp.where(near, xs * half - 1 + n_tp - 1, xs * half))

    def send_row(row, peer, box, recv_sem):
        pltpu.make_async_remote_copy(
            src_ref=msg.at[row],
            dst_ref=box.at[dp],
            send_sem=dp_send,
            recv_sem=recv_sem,
            device_id={"dp": peer},
            device_id_type=MESH,
        ).start()

    for peer, _ in near_peers:
        send_row(peer, peer, inbox, dp_recv)

    @pl.when(far)
    def _():
        peer, behind = own_column
        pl.semaphore_signal(entered, inc=1, device_id={"dp": partner}, device_id_type=MESH)
        send_row(peer, peer, inbox, dp_recv)
        send_row(behind, peer, relay, relay_recv)

    for peer, behind in near_peers:
        send_row(behind, peer, relay, relay_recv)

    shifted = jnp.pad((ids_v[...] - tp * vocab).astype(F32), ((0, 6), (0, 0)))
    idt[...] = jnp.transpose(shifted).astype(jnp.int32)
    stt[...] = jnp.zeros((128, 128), F32)
    lane = lax.broadcasted_iota(jnp.int32, (BLOCK, 128), 1)
    for b in range(2):
        for h in range(2):
            chunks[b * 2 + h].wait()

            def token_block(i, carry):
                rows = pl.ds(pl.multiple_of(h * 64 + i * BLOCK, BLOCK), BLOCK)
                top = lg[b, rows, pl.ds(0, 128)]
                for c in range(1, vocab // 128):
                    top = jnp.maximum(top, lg[b, rows, pl.ds(c * 128, 128)])
                top = jnp.max(top.astype(F32), axis=1, keepdims=True)
                tops = jnp.broadcast_to(top, (BLOCK, 128))
                wanted = jnp.broadcast_to(idt[rows, b : b + 1], (BLOCK, 128))
                total = jnp.zeros((BLOCK, 128), F32)
                found = jnp.zeros((BLOCK, 128), F32)
                for c in range(vocab // 128):
                    x = lg[b, rows, pl.ds(c * 128, 128)].astype(F32)
                    total = total + jnp.exp(x - tops)
                    found = jnp.where(wanted == lane + c * 128, x, found)
                stt[rows, b : b + 1] = top
                stt[rows, 2 + b : 3 + b] = jnp.sum(total, axis=1, keepdims=True)
                stt[rows, 4 + b : 5 + b] = jnp.sum(found, axis=1, keepdims=True)
                return carry

            lax.fori_loop(0, 64 // BLOCK, token_block, 0)
    t1_src[0:6] = jnp.transpose(stt[...])[0:6]
    t1_src[6:8] = jnp.concatenate(parts, axis=0)
    t1[pl.ds(tp, 1)] = t1_src[...][None]

    def send_tensor(src, dst, send_sem, recv_sem):
        for peer in tp_peers:
            pltpu.make_async_remote_copy(
                src_ref=src,
                dst_ref=dst.at[tp],
                send_sem=send_sem,
                recv_sem=recv_sem,
                device_id={"tensor": peer},
                device_id_type=MESH,
            ).start()

    def first(ref, rows, sem):
        some = ref.at[pl.ds(0, rows)]
        return pltpu.make_async_copy(some, some, sem)

    @pl.when(near)
    def _():
        send_tensor(t1_src, t1, t1_send, t1_recv)
        first(inbox, n_dp - 1, dp_recv).wait()

    @pl.when(far)
    def _():
        first(inbox, n_dp, dp_recv).wait()
        send_tensor(t1_src, t1, t1_send, t1_recv)

    got = inbox[...][:, 0, :]
    quiet[pl.ds(0, 64, stride=2), :] = got
    quiet[pl.ds(1, 64, stride=2), :] = pltpu.roll(got, 127, 1)
    turned = jnp.transpose(quiet[...])

    def pair(k):
        return jnp.concatenate([turned[k : k + 1], turned[16 + k : 17 + k]], axis=0)

    t2_src[...] = pair(0)
    t2[pl.ds(tp, 1)] = t2_src[...][None]

    send_tensor(t2_src, t2, t2_send, t2_recv)

    @pl.when(near)
    def _():
        pl.semaphore_wait(entered, 1)
        for peer in tp_peers:
            pl.semaphore_signal(line_in, inc=1, device_id={"tensor": peer}, device_id_type=MESH)

    ref_rows, held_returns = pair(2), pair(4)
    same = (turned[12:13] == pid).astype(F32)
    count = jnp.sum(same * turned[6:7], axis=1, keepdims=True)
    summed = jnp.sum(same * turned[8:9], axis=1, keepdims=True)
    square = jnp.sum(same * turned[10:11], axis=1, keepdims=True)
    floor = jnp.maximum(count, 1.0)
    mean = summed / floor
    var = (square - mean * summed) / floor
    whitened = (advantages - mean) * lax.rsqrt(var + 1.0)

    first(t1, n_tp - 1, t1_recv).wait()
    shards = t1[...]
    values = jnp.sum(shards[:, 6:8], axis=0)
    coeff = jnp.where(held_returns > 1e29, 0.0, 32.0 * (values - held_returns))
    for j in range(2):
        grad_out[j] = (w_all * coeff[j : j + 1]).astype(jnp.bfloat16)

    tops = shards[:, 0:2]
    row_max = jnp.max(tops, axis=0)
    total = jnp.sum(shards[:, 2:4] * jnp.exp(tops - row_max[None]), axis=0)
    target = jnp.sum(shards[:, 4:6], axis=0)
    logprob = target - (row_max + jnp.log(total))
    ratio = jnp.exp(jnp.clip(logprob - old_v[...], -20.0, 20.0))
    surrogate = jnp.maximum(-whitened * ratio, -whitened * jnp.clip(ratio, 0.8, 1.2))
    surrogate = jnp.where(whitened < 0.0, jnp.minimum(surrogate, -3.0 * whitened), surrogate)
    drift = jnp.clip(ref_rows - logprob, -20.0, 20.0)
    penalty = jnp.clip(jnp.exp(drift) - drift - 1.0, -10.0, 10.0)
    policy = live * (surrogate + 0.1 * penalty)
    scale = 0.25 * live

    forward = pltpu.make_async_remote_copy(
        src_ref=relay,
        dst_ref=inbox,
        send_sem=relay_send,
        recv_sem=dp_recv,
        device_id={"dp": partner},
        device_id_type=MESH,
    )

    @pl.when(near)
    def _():
        pl.semaphore_wait(line_in, n_tp - 1)
        first(relay, n_dp - 1, relay_recv).wait()
        forward.start()

    first(t2, n_tp - 1, t2_recv).wait()
    error = jnp.sum(t2[...], axis=0) - returns
    loss_out[...] = policy + scale * error * error

    first(t1, n_tp - 1, t1_send).wait()
    first(t2, n_tp - 1, t2_send).wait()

    @pl.when(near)
    def _():
        first(msg, n_dp - 2, dp_send).wait()
        first(relay, n_dp, relay_send).wait()

    @pl.when(far)
    def _():
        first(msg, n_dp, dp_send).wait()


def finish(loss, grad, loss_out, grad_out, sems):
    copies = [
        pltpu.make_async_copy(src, dst, sems.at[n])
        for n, (src, dst) in enumerate([(grad, grad_out), (loss, loss_out)])
    ]
    for copy in copies:
        copy.start()
    for copy in copies:
        copy.wait()


def per_device(sizes, *arrays):
    (
        logits, ids, mask, lengths, prompt_of, old, ref, adv, ret, critic, weight
    ) = arrays
    seqs, length, vocab = logits.shape
    batch, tile, feats = critic.shape
    xs, zs, ys = sizes
    any_ref, vmem = pl.BlockSpec(memory_space=pl.ANY), pl.BlockSpec(memory_space=pltpu.VMEM)
    dma = pltpu.SemaphoreType.DMA
    vm = pltpu.VMEM
    loss, grad = pl.pallas_call(
        functools.partial(kernel, xs, zs, ys, vocab),
        out_shape=(
            vm((seqs, length), F32),
            vm((tile, feats, batch), jnp.bfloat16),
        ),
        in_specs=[any_ref] * 11,
        out_specs=[vmem] * 2,
        scratch_shapes=[
            vm(logits.shape, jnp.bfloat16),
            vm((tile, feats, batch), jnp.bfloat16),
            vm((seqs, length), jnp.int32),
            vm((seqs, length), jnp.int32),
            vm((seqs, length), F32),
            vm((tile, batch), jnp.bfloat16),
            vm((seqs, length), F32),
            vm((seqs, length), F32),
            vm((feats,), jnp.bfloat16),
            pltpu.SMEM((seqs,), jnp.int32),
            pltpu.SMEM((seqs,), jnp.int32),
            vm((128, 128), F32),
            vm((64, 1, 128), F32),
            vm((64, 1, 128), F32),
            vm((64, 1, 128), F32),
            vm((128, 128), F32),
            vm((128, 8), jnp.int32),
            vm((128, 128), F32),
            vm((8, 128), F32),
            vm((2 * ys, 8, 128), F32),
            vm((seqs, length), F32),
            vm((2 * ys, seqs, length), F32),
            dma((4,)), dma((10,)), dma, dma, dma, dma, dma, dma,
            dma, dma, pltpu.SemaphoreType.REGULAR, pltpu.SemaphoreType.REGULAR,
        ],
        compiler_params=pltpu.CompilerParams(collective_id=0, has_side_effects=True),
        name="ppo_all",
    )(
        logits, ids, mask, lengths, prompt_of, old, ref.T, adv, ret,
        jnp.transpose(critic, (1, 2, 0)), weight,
    )
    loss, grad = pl.pallas_call(
        finish,
        out_shape=(
            jax.ShapeDtypeStruct((seqs, length), F32),
            jax.ShapeDtypeStruct((tile, feats, batch), jnp.bfloat16),
        ),
        in_specs=[vmem] * 2,
        out_specs=[any_ref] * 2,
        scratch_shapes=[dma((2,))],
        compiler_params=pltpu.CompilerParams(vmem_limit_bytes=2**20),
        name="ppo_finish",
    )(loss, grad)
    return loss, jnp.transpose(grad, (2, 0, 1))


def solution(mesh):
    in_specs = (
        P("dp", None, "tensor"),
        P("dp", None),
        P("dp", None),
        P("dp"),
        P("dp"),
        P("dp", None),
        P(None, "dp"),
        P("dp", None),
        P("dp", None),
        P(None, "dp", "tensor"),
        P("tensor"),
    )
    out_specs = (P("dp", None), P(None, "dp", "tensor"))
    dp_size, tp_size = mesh.shape["dp"], mesh.shape["tensor"]
    sizes = (4, dp_size // 4, tp_size // 2)
    return jax.shard_map(
        functools.partial(per_device, sizes),
        mesh=mesh,
        in_specs=in_specs,
        out_specs=out_specs,
        check_vma=False,
    )
```

```python
import functools
import itertools

import jax
import jax.numpy as jnp
from jax import lax
from jax.experimental import pallas as pl
from jax.experimental.pallas import tpu as pltpu
from jax.sharding import PartitionSpec as P

MESH = pl.DeviceIdType.MESH
F32 = jnp.float32
DEAD = 1e30
BLOCK = 16


def far_first(*sizes):
    offsets = itertools.product(*(range(n) for n in sizes))
    return sorted(offsets, key=lambda o: -sum(min(d, n - d) for d, n in zip(o, sizes)))[:-1]


def kernel(
    xs, zs, ys, vocab,
    logits, ids, mask, lengths_in, prompt_in, old, ref_t, adv, ret, critic, weight,
    loss_out, grad_out,
    lg, cr, ids_v, mask_v, old_v, ref_v, adv_v, ret_v, w_v, lengths, prompt_of,
    stage, msg, inbox, relay, direct, quiet, idt, stt, t1_src, t1, t2_src, t2,
    lg_sem, in_sem, dp_send, dp_recv, t1_send, t1_recv, t2_send, t2_recv,
    relay_send, relay_recv, direct_send, direct_recv, entered, line_in,
):
    dp, tp = lax.axis_index("dp"), lax.axis_index("tensor")
    n_dp, n_tp = xs * zs, 2 * ys
    my_x, my_z, my_y, my_c = dp // zs, lax.rem(dp, zs), tp // 2, lax.rem(tp, 2)

    smalls = [
        pltpu.make_async_copy(src, dst, in_sem.at[n])
        for n, (src, dst) in enumerate(
            [
                *((critic.at[j, r], cr.at[j, r]) for j in range(2) for r in (pl.ds(0, 160), pl.ds(160, 160))),
                (weight, w_v), (ref_t, ref_v), (mask, mask_v), (adv, adv_v),
                (lengths_in, lengths), (prompt_in, prompt_of), (ret, ret_v), (ids, ids_v), (old, old_v),
            ]
        )
    ]
    for copy in smalls:
        copy.start()
    at_x = [lax.rem(my_x + d, xs) * zs for d in range(xs)]
    at_z = [lax.rem(my_z + d, zs) for d in range(zs)]
    at_y = [lax.rem(my_y + d, ys) * 2 for d in range(ys)]
    at_c = [my_c, 1 - my_c]
    dp_peers = [at_x[x] + at_z[z] for x, z in far_first(xs, zs)]
    half = zs // 2
    near, far = my_z < half, my_z >= half
    partner = my_x * zs + (zs - 1 - my_z)
    at_near = [lax.rem(my_z + d, half) for d in range(half)]
    near_peers = [
        (at_x[x] + at_near[z], at_x[x] + (zs - 1 - at_near[z])) for x, z in far_first(xs, half)
    ]
    low, high = ys // 2 - 1, ys // 2 + 1
    straight = jnp.logical_and(my_y >= low, my_y <= high)
    in_low, in_high = 2 * low, 2 * high + 2
    first_dp, first_tp = 0, 1
    is_first = jnp.logical_and(dp == first_dp, tp == first_tp)
    skips = jnp.logical_and(dp == first_dp, straight)
    columns = [(z, x) for z in range(half) for x in sorted(range(xs), key=lambda d: -min(d, xs - d))]
    tp_peers = [at_y[y] + at_c[c] for y, c in far_first(ys, 2)]

    barrier = pltpu.get_barrier_semaphore()

    @pl.when(near)
    def _():
        for peer in dp_peers:
            pl.semaphore_signal(barrier, inc=1, device_id={"dp": peer}, device_id_type=MESH)
        for peer in tp_peers:
            pl.semaphore_signal(barrier, inc=1, device_id={"tensor": peer}, device_id_type=MESH)

    @pl.when(is_first)
    def _():
        for column in range(in_low, in_high):

            def greet(i, carry):
                place = {"dp": i, "tensor": column}
                pl.semaphore_signal(barrier, inc=1, device_id=place, device_id_type=MESH)
                return carry

            lax.fori_loop(1, n_dp, greet, 0)

    for copy in smalls:
        copy.wait()
    chunks = []
    for b in range(2):
        for h in range(2):
            rows = pl.ds(h * 64, 64)
            chunks.append(
                pltpu.make_async_copy(logits.at[b, rows], lg.at[b, rows], lg_sem.at[b * 2 + h])
            )
            chunks[-1].start()

    row2 = lax.broadcasted_iota(jnp.int32, (2, 128), 0)
    lane2 = lax.broadcasted_iota(jnp.int32, (2, 128), 1)
    length_of = jnp.where(row2 == 0, lengths[0], lengths[1])
    live = (mask_v[...] * (lane2 < length_of).astype(jnp.int32)).astype(F32)
    advantages, returns = adv_v[...], ret_v[...]
    live_adv = live * advantages

    def spread(column):
        return jnp.broadcast_to(jnp.sum(column, axis=1, keepdims=True), (2, 128))

    feats = w_v.shape[0]
    w_row = jnp.pad(w_v[...].astype(F32).reshape(1, feats), ((0, 0), (0, -feats % 128)))
    w_all = jnp.transpose(jnp.broadcast_to(w_row, (128, w_row.shape[1])))[:feats]
    parts = [
        jnp.sum(cr[j].astype(F32) * w_all, axis=0, keepdims=True) for j in range(2)
    ]
    pid = jnp.where(row2 == 0, prompt_of[0], prompt_of[1]).astype(F32)
    lines = jnp.concatenate(
        parts
        + [
            ref_v[...].astype(F32),
            jnp.where(live > 0.0, returns, DEAD),
            spread(live),
            spread(live_adv),
            spread(live_adv * advantages),
            pid,
            jnp.zeros((114, 128), F32),
        ],
        axis=0,
    )
    stage[...] = jnp.transpose(lines)
    packed = stage[pl.ds(0, 64, stride=2), :] + pltpu.roll(stage[pl.ds(1, 64, stride=2), :], 16, 1)
    msg[...] = packed[:, None, :]

    def read_logits():
        shifted = jnp.pad((ids_v[...] - tp * vocab).astype(F32), ((0, 6), (0, 0)))
        idt[...] = jnp.transpose(shifted).astype(jnp.int32)
        stt[...] = jnp.zeros((128, 128), F32)
        lane = lax.broadcasted_iota(jnp.int32, (BLOCK, 128), 1)
        for b in range(2):
            for h in range(2):
                chunks[b * 2 + h].wait()

                def token_block(i, carry):
                    rows = pl.ds(pl.multiple_of(h * 64 + i * BLOCK, BLOCK), BLOCK)
                    top = lg[b, rows, pl.ds(0, 128)]
                    for c in range(1, vocab // 128):
                        top = jnp.maximum(top, lg[b, rows, pl.ds(c * 128, 128)])
                    top = jnp.max(top.astype(F32), axis=1, keepdims=True)
                    tops = jnp.broadcast_to(top, (BLOCK, 128))
                    wanted = jnp.broadcast_to(idt[rows, b : b + 1], (BLOCK, 128))
                    total = jnp.zeros((BLOCK, 128), F32)
                    found = jnp.zeros((BLOCK, 128), F32)
                    for c in range(vocab // 128):
                        x = lg[b, rows, pl.ds(c * 128, 128)].astype(F32)
                        total = total + jnp.exp(x - tops)
                        found = jnp.where(wanted == lane + c * 128, x, found)
                    stt[rows, b : b + 1] = top
                    stt[rows, 2 + b : 3 + b] = jnp.sum(total, axis=1, keepdims=True)
                    stt[rows, 4 + b : 5 + b] = jnp.sum(found, axis=1, keepdims=True)
                    return carry

                lax.fori_loop(0, 64 // BLOCK, token_block, 0)
        t1_src[0:6] = jnp.transpose(stt[...])[0:6]
        t1_src[6:8] = jnp.concatenate(parts, axis=0)
        t1[pl.ds(tp, 1)] = t1_src[...][None]

    @pl.when(near)
    def _():
        inbox[pl.ds(dp, 1)] = msg[pl.ds(dp, 1)]
        relay[pl.ds(dp, 1)] = msg[pl.ds(partner, 1)]

    @pl.when(my_z < half // 2)
    def _():
        read_logits()

    guests = jnp.where(near, xs * half - 1 + n_tp - 1, xs * half)
    pl.semaphore_wait(barrier, guests + jnp.where(straight, 1, 0) - jnp.where(skips, 1, 0))

    def send_row(row, peer, box, recv_sem):
        pltpu.make_async_remote_copy(
            src_ref=msg.at[row],
            dst_ref=box.at[dp],
            send_sem=dp_send,
            recv_sem=recv_sem,
            device_id={"dp": peer},
            device_id_type=MESH,
        ).start()

    @pl.when(straight)
    def _():
        pltpu.make_async_remote_copy(
            src_ref=msg.at[first_dp],
            dst_ref=direct.at[tp - in_low, dp],
            send_sem=direct_send,
            recv_sem=direct_recv,
            device_id={"dp": first_dp, "tensor": first_tp},
            device_id_type=MESH,
        ).start()

    @pl.when(far)
    def _():
        pl.semaphore_signal(entered, inc=1, device_id={"dp": partner}, device_id_type=MESH)
        for z, x in columns:
            send_row(at_x[x] + z, at_x[x] + z, inbox, dp_recv)
        for z, x in columns:
            send_row(at_x[x] + zs - 1 - z, at_x[x] + z, relay, relay_recv)

    @pl.when(near)
    def _():
        for peer, _ in near_peers:
            send_row(peer, peer, inbox, dp_recv)
        for peer, behind in near_peers:
            send_row(behind, peer, relay, relay_recv)

    @pl.when(my_z >= half // 2)
    def _():
        read_logits()

    def send_one(src, dst, send_sem, recv_sem, peer):
        pltpu.make_async_remote_copy(
            src_ref=src,
            dst_ref=dst.at[tp],
            send_sem=send_sem,
            recv_sem=recv_sem,
            device_id={"tensor": peer},
            device_id_type=MESH,
        ).start()

    def send_t1():
        for peer in tp_peers:
            send_one(t1_src, t1, t1_send, t1_recv, peer)

    def first(ref, rows, sem):
        some = ref.at[pl.ds(0, rows)]
        return pltpu.make_async_copy(some, some, sem)

    @pl.when(near)
    def _():
        send_t1()
        pl.semaphore_wait(entered, 1)
        for peer in tp_peers:
            pl.semaphore_signal(line_in, inc=1, device_id={"tensor": peer}, device_id_type=MESH)
        first(inbox, n_dp - 1, dp_recv).wait()

    @pl.when(far)
    def _():
        first(inbox, n_dp, dp_recv).wait()
        send_t1()

    def turn(got):
        quiet[pl.ds(0, 64, stride=2), :] = got
        quiet[pl.ds(1, 64, stride=2), :] = pltpu.roll(got, 127, 1)
        return jnp.transpose(quiet[...])

    def pair(turned, k):
        return jnp.concatenate([turned[k : k + 1], turned[16 + k : 17 + k]], axis=0)

    turned = turn(inbox[...][:, 0, :])
    t2_src[...] = pair(turned, 0)
    t2[pl.ds(tp, 1)] = t2_src[...][None]

    for peer in tp_peers:

        @pl.when(jnp.logical_not(jnp.logical_and(skips, peer == first_tp)))
        def _():
            send_one(t2_src, t2, t2_send, t2_recv, peer)


    forward = pltpu.make_async_remote_copy(
        src_ref=relay,
        dst_ref=inbox,
        send_sem=relay_send,
        recv_sem=dp_recv,
        device_id={"dp": partner},
        device_id_type=MESH,
    )

    @pl.when(near)
    def _():
        pl.semaphore_wait(line_in, n_tp - 1)
        first(relay, n_dp - 1, relay_recv).wait()
        forward.start()

    ref_rows, held_returns = pair(turned, 2), pair(turned, 4)
    same = (turned[12:13] == pid).astype(F32)
    count = jnp.sum(same * turned[6:7], axis=1, keepdims=True)
    summed = jnp.sum(same * turned[8:9], axis=1, keepdims=True)
    square = jnp.sum(same * turned[10:11], axis=1, keepdims=True)
    floor = jnp.maximum(count, 1.0)
    mean = summed / floor
    var = (square - mean * summed) / floor
    whitened = (advantages - mean) * lax.rsqrt(var + 1.0)

    first(t1, n_tp - 1, t1_recv).wait()
    shards = t1[...]
    values = jnp.sum(shards[:, 6:8], axis=0)
    coeff = jnp.where(held_returns > 1e29, 0.0, 32.0 * (values - held_returns))
    for j in range(2):
        grad_out[j] = (w_all * coeff[j : j + 1]).astype(jnp.bfloat16)

    tops = shards[:, 0:2]
    row_max = jnp.max(tops, axis=0)
    total = jnp.sum(shards[:, 2:4] * jnp.exp(tops - row_max[None]), axis=0)
    target = jnp.sum(shards[:, 4:6], axis=0)
    logprob = target - (row_max + jnp.log(total))
    ratio = jnp.exp(jnp.clip(logprob - old_v[...], -20.0, 20.0))
    surrogate = jnp.maximum(-whitened * ratio, -whitened * jnp.clip(ratio, 0.8, 1.2))
    surrogate = jnp.where(whitened < 0.0, jnp.minimum(surrogate, -3.0 * whitened), surrogate)
    drift = jnp.clip(ref_rows - logprob, -20.0, 20.0)
    penalty = jnp.clip(jnp.exp(drift) - drift - 1.0, -10.0, 10.0)
    policy = live * (surrogate + 0.1 * penalty)
    scale = 0.25 * live

    @pl.when(is_first)
    def _():
        first(t2, n_tp - 1 - (in_high - in_low), t2_recv).wait()
        pltpu.make_async_copy(direct, direct, direct_recv).wait()
        t2[in_low] = pair(turn(jnp.sum(direct[...], axis=0)[:, 0, :]), 0)
        for column in range(in_low + 1, in_high):
            t2[column] = jnp.zeros((2, 128), F32)

    @pl.when(jnp.logical_not(is_first))
    def _():
        first(t2, n_tp - 1, t2_recv).wait()

    error = jnp.sum(t2[...], axis=0) - returns
    loss_out[...] = policy + scale * error * error

    first(t1, n_tp - 1, t1_send).wait()

    @pl.when(skips)
    def _():
        first(t2, n_tp - 2, t2_send).wait()

    @pl.when(jnp.logical_not(skips))
    def _():
        first(t2, n_tp - 1, t2_send).wait()

    @pl.when(straight)
    def _():
        first(msg, 1, direct_send).wait()

    @pl.when(near)
    def _():
        first(msg, n_dp - 2, dp_send).wait()
        first(relay, n_dp, relay_send).wait()

    @pl.when(far)
    def _():
        first(msg, n_dp, dp_send).wait()


def finish(loss, grad, loss_out, grad_out, sems):
    copies = [
        pltpu.make_async_copy(src, dst, sems.at[n])
        for n, (src, dst) in enumerate([(grad, grad_out), (loss, loss_out)])
    ]
    for copy in copies:
        copy.start()
    for copy in copies:
        copy.wait()


def per_device(sizes, *arrays):
    (
        logits, ids, mask, lengths, prompt_of, old, ref, adv, ret, critic, weight
    ) = arrays
    seqs, length, vocab = logits.shape
    batch, tile, feats = critic.shape
    xs, zs, ys = sizes
    any_ref, vmem = pl.BlockSpec(memory_space=pl.ANY), pl.BlockSpec(memory_space=pltpu.VMEM)
    dma = pltpu.SemaphoreType.DMA
    vm = pltpu.VMEM
    loss, grad = pl.pallas_call(
        functools.partial(kernel, xs, zs, ys, vocab),
        out_shape=(
            vm((seqs, length), F32),
            vm((tile, feats, batch), jnp.bfloat16),
        ),
        in_specs=[any_ref] * 11,
        out_specs=[vmem] * 2,
        scratch_shapes=[
            vm(logits.shape, jnp.bfloat16),
            vm((tile, feats, batch), jnp.bfloat16),
            vm((seqs, length), jnp.int32),
            vm((seqs, length), jnp.int32),
            vm((seqs, length), F32),
            vm((tile, batch), jnp.bfloat16),
            vm((seqs, length), F32),
            vm((seqs, length), F32),
            vm((feats,), jnp.bfloat16),
            pltpu.SMEM((seqs,), jnp.int32),
            pltpu.SMEM((seqs,), jnp.int32),
            vm((128, 128), F32),
            vm((64, 1, 128), F32),
            vm((64, 1, 128), F32),
            vm((64, 1, 128), F32),
            vm((6, 64, 1, 128), F32),
            vm((128, 128), F32),
            vm((128, 8), jnp.int32),
            vm((128, 128), F32),
            vm((8, 128), F32),
            vm((2 * ys, 8, 128), F32),
            vm((seqs, length), F32),
            vm((2 * ys, seqs, length), F32),
            dma((4,)), dma((13,)), dma, dma, dma, dma, dma, dma,
            dma, dma, dma, dma, pltpu.SemaphoreType.REGULAR, pltpu.SemaphoreType.REGULAR,
        ],
        compiler_params=pltpu.CompilerParams(collective_id=0, has_side_effects=True),
        name="ppo_all",
    )(
        logits, ids, mask, lengths, prompt_of, old, ref.T, adv, ret,
        jnp.transpose(critic, (1, 2, 0)), weight,
    )
    loss, grad = pl.pallas_call(
        finish,
        out_shape=(
            jax.ShapeDtypeStruct((seqs, length), F32),
            jax.ShapeDtypeStruct((tile, feats, batch), jnp.bfloat16),
        ),
        in_specs=[vmem] * 2,
        out_specs=[any_ref] * 2,
        scratch_shapes=[dma((2,))],
        compiler_params=pltpu.CompilerParams(vmem_limit_bytes=2**20),
        name="ppo_finish",
    )(loss, grad)
    return loss, jnp.transpose(grad, (2, 0, 1))


def solution(mesh):
    in_specs = (
        P("dp", None, "tensor"),
        P("dp", None),
        P("dp", None),
        P("dp"),
        P("dp"),
        P("dp", None),
        P(None, "dp"),
        P("dp", None),
        P("dp", None),
        P(None, "dp", "tensor"),
        P("tensor"),
    )
    out_specs = (P("dp", None), P(None, "dp", "tensor"))
    dp_size, tp_size = mesh.shape["dp"], mesh.shape["tensor"]
    sizes = (4, dp_size // 4, tp_size // 2)
    return jax.shard_map(
        functools.partial(per_device, sizes),
        mesh=mesh,
        in_specs=in_specs,
        out_specs=out_specs,
        check_vma=False,
    )
```

```python
import functools
import itertools

import jax
import jax.numpy as jnp
from jax import lax
from jax.experimental import pallas as pl
from jax.experimental.pallas import tpu as pltpu
from jax.sharding import PartitionSpec as P

MESH = pl.DeviceIdType.MESH
F32 = jnp.float32
DEAD = 1e30
BLOCK = 16


def far_first(*sizes):
    offsets = itertools.product(*(range(n) for n in sizes))
    return sorted(offsets, key=lambda o: -sum(min(d, n - d) for d, n in zip(o, sizes)))[:-1]


def kernel(
    xs, zs, ys, vocab,
    logits, ids, mask, lengths_in, prompt_in, old, ref_t, adv, ret, critic, weight,
    loss_out, grad_out,
    lg, cr, ids_v, mask_v, old_v, ref_v, adv_v, ret_v, w_v, lengths, prompt_of,
    stage, msg, inbox, relay, block, direct, quiet, idt, stt, t1_src, t1, t2_src, t2,
    lg_sem, in_sem, dp_send, dp_recv, t1_send, t1_recv, t2_send, t2_recv,
    relay_send, block_recv, direct_send, direct_recv, entered, line_in,
):
    dp, tp = lax.axis_index("dp"), lax.axis_index("tensor")
    n_dp, n_tp = xs * zs, 2 * ys
    my_x, my_z, my_y, my_c = dp // zs, lax.rem(dp, zs), tp // 2, lax.rem(tp, 2)

    smalls = [
        pltpu.make_async_copy(src, dst, in_sem.at[n])
        for n, (src, dst) in enumerate(
            [
                *((critic.at[j, r], cr.at[j, r]) for j in range(2) for r in (pl.ds(0, 160), pl.ds(160, 160))),
                (weight, w_v), (ref_t, ref_v), (mask, mask_v), (adv, adv_v),
                (lengths_in, lengths), (prompt_in, prompt_of), (ret, ret_v), (ids, ids_v), (old, old_v),
            ]
        )
    ]
    for copy in smalls:
        copy.start()
    at_x = [lax.rem(my_x + d, xs) * zs for d in range(xs)]
    at_z = [lax.rem(my_z + d, zs) for d in range(zs)]
    at_y = [lax.rem(my_y + d, ys) * 2 for d in range(ys)]
    at_c = [my_c, 1 - my_c]
    dp_peers = [at_x[x] + at_z[z] for x, z in far_first(xs, zs)]
    half = zs // 2
    near, far = my_z < half, my_z >= half
    partner = my_x * zs + (zs - 1 - my_z)
    at_near = [lax.rem(my_z + d, half) for d in range(half)]
    near_peers = [(at_x[x] + at_near[z], at_x[x] // 2 + at_near[z]) for x, z in far_first(xs, half)]
    low, high = ys // 2 - 1, ys // 2 + 2
    first_dp, first_tp = 0, 1
    in_low, in_high = 2 * low, 2 * high + 2
    afar = jnp.logical_and(my_y >= low, my_y <= high)
    straight = jnp.logical_or(afar, tp == 0)
    sources = [0, *range(in_low, in_high)]
    is_first = jnp.logical_and(dp == first_dp, tp == first_tp)
    skips = jnp.logical_and(dp == first_dp, straight)
    columns = [(z, x) for z in range(half) for x in sorted(range(xs), key=lambda d: -min(d, xs - d))]
    tp_peers = [at_y[y] + at_c[c] for y, c in far_first(ys, 2)]

    barrier = pltpu.get_barrier_semaphore()

    @pl.when(near)
    def _():
        for peer in dp_peers:
            pl.semaphore_signal(barrier, inc=1, device_id={"dp": peer}, device_id_type=MESH)
        for peer in tp_peers:
            pl.semaphore_signal(barrier, inc=1, device_id={"tensor": peer}, device_id_type=MESH)

    @pl.when(is_first)
    def _():
        for column in sources:

            def greet(i, carry):
                place = {"dp": i, "tensor": column}
                pl.semaphore_signal(barrier, inc=1, device_id=place, device_id_type=MESH)
                return carry

            lax.fori_loop(1, n_dp, greet, 0)

    for copy in smalls:
        copy.wait()
    chunks = []
    for b in range(2):
        for h in range(2):
            rows = pl.ds(h * 64, 64)
            chunks.append(
                pltpu.make_async_copy(logits.at[b, rows], lg.at[b, rows], lg_sem.at[b * 2 + h])
            )
            chunks[-1].start()

    row2 = lax.broadcasted_iota(jnp.int32, (2, 128), 0)
    lane2 = lax.broadcasted_iota(jnp.int32, (2, 128), 1)
    length_of = jnp.where(row2 == 0, lengths[0], lengths[1])
    live = (mask_v[...] * (lane2 < length_of).astype(jnp.int32)).astype(F32)
    advantages, returns = adv_v[...], ret_v[...]
    live_adv = live * advantages

    def spread(column):
        return jnp.broadcast_to(jnp.sum(column, axis=1, keepdims=True), (2, 128))

    feats = w_v.shape[0]
    w_row = w_v[...].reshape(1, feats)
    parts = [
        jnp.dot(jnp.broadcast_to(w_row, (16, feats)), cr[j], preferred_element_type=F32)[:1]
        for j in range(2)
    ]
    pid = jnp.where(row2 == 0, prompt_of[0], prompt_of[1]).astype(F32)
    lines = jnp.concatenate(
        parts
        + [
            ref_v[...].astype(F32),
            jnp.where(live > 0.0, returns, DEAD),
            spread(live),
            spread(live_adv),
            spread(live_adv * advantages),
            pid,
            jnp.zeros((114, 128), F32),
        ],
        axis=0,
    )
    stage[...] = jnp.transpose(lines)
    packed = stage[pl.ds(0, 64, stride=2), :] + pltpu.roll(stage[pl.ds(1, 64, stride=2), :], 16, 1)
    for x in range(xs):
        for z in range(half):
            for side, row in enumerate((x * zs + z, x * zs + zs - 1 - z)):
                msg[x * half + z, side : side + 1] = packed[row : row + 1]

    def read_logits():
        shifted = jnp.pad((ids_v[...] - tp * vocab).astype(F32), ((0, 6), (0, 0)))
        idt[...] = jnp.transpose(shifted).astype(jnp.int32)
        stt[...] = jnp.zeros((128, 128), F32)
        lane = lax.broadcasted_iota(jnp.int32, (BLOCK, 128), 1)
        for b in range(2):
            for h in range(2):
                chunks[b * 2 + h].wait()

                def token_block(i, carry):
                    rows = pl.ds(pl.multiple_of(h * 64 + i * BLOCK, BLOCK), BLOCK)
                    top = lg[b, rows, pl.ds(0, 128)]
                    for c in range(1, vocab // 128):
                        top = jnp.maximum(top, lg[b, rows, pl.ds(c * 128, 128)])
                    top = jnp.max(top.astype(F32), axis=1, keepdims=True)
                    tops = jnp.broadcast_to(top, (BLOCK, 128))
                    wanted = jnp.broadcast_to(idt[rows, b : b + 1], (BLOCK, 128))
                    total = jnp.zeros((BLOCK, 128), F32)
                    found = jnp.zeros((BLOCK, 128), F32)
                    for c in range(vocab // 128):
                        x = lg[b, rows, pl.ds(c * 128, 128)].astype(F32)
                        total = total + jnp.exp(x - tops)
                        found = jnp.where(wanted == lane + c * 128, x, found)
                    stt[rows, b : b + 1] = top
                    stt[rows, 2 + b : 3 + b] = jnp.sum(total, axis=1, keepdims=True)
                    stt[rows, 4 + b : 5 + b] = jnp.sum(found, axis=1, keepdims=True)
                    return carry

                lax.fori_loop(0, 64 // BLOCK, token_block, 0)
        t1_src[0:6] = jnp.transpose(stt[...])[0:6]
        t1_src[6:8] = jnp.concatenate(parts, axis=0)
        t1[pl.ds(tp, 1)] = t1_src[...][None]

    @pl.when(near)
    def _():
        inbox[pl.ds(dp, 1)] = msg[pl.ds(my_x * half + my_z, 1)]

    @pl.when(my_z < half // 2)
    def _():
        read_logits()

    guests = jnp.where(near, xs * half - 1 + n_tp - 1, xs * half)
    pl.semaphore_wait(barrier, guests + jnp.where(straight, 1, 0) - jnp.where(skips, 1, 0))

    def send_rows(place, peer):
        pltpu.make_async_remote_copy(
            src_ref=msg.at[place],
            dst_ref=inbox.at[dp],
            send_sem=dp_send,
            recv_sem=dp_recv,
            device_id={"dp": peer},
            device_id_type=MESH,
        ).start()

    @pl.when(straight)
    def _():
        pltpu.make_async_remote_copy(
            src_ref=msg.at[first_dp],
            dst_ref=direct.at[jnp.where(afar, tp - in_low + 1, 0), dp],
            send_sem=direct_send,
            recv_sem=direct_recv,
            device_id={"dp": first_dp, "tensor": first_tp},
            device_id_type=MESH,
        ).start()

    @pl.when(far)
    def _():
        pl.semaphore_signal(entered, inc=1, device_id={"dp": partner}, device_id_type=MESH)
        for z, x in columns:
            send_rows(at_x[x] // 2 + z, at_x[x] + z)

    @pl.when(near)
    def _():
        for peer, place in near_peers:
            send_rows(place, peer)

    @pl.when(my_z >= half // 2)
    def _():
        read_logits()

    def take(got):
        quiet[pl.ds(0, 64, stride=2), :] = got
        quiet[pl.ds(1, 64, stride=2), :] = pltpu.roll(got, 127, 1)

    def send_one(src, dst, send_sem, recv_sem, peer):
        pltpu.make_async_remote_copy(
            src_ref=src,
            dst_ref=dst.at[tp],
            send_sem=send_sem,
            recv_sem=recv_sem,
            device_id={"tensor": peer},
            device_id_type=MESH,
        ).start()

    def send_t1():
        for peer in tp_peers:
            send_one(t1_src, t1, t1_send, t1_recv, peer)

    def first(ref, rows, sem):
        some = ref.at[pl.ds(0, rows)]
        return pltpu.make_async_copy(some, some, sem)

    @pl.when(near)
    def _():
        send_t1()
        pl.semaphore_wait(entered, 1)
        for peer in tp_peers:
            pl.semaphore_signal(line_in, inc=1, device_id={"tensor": peer}, device_id_type=MESH)
        first(inbox, n_dp - 1, dp_recv).wait()
        take(inbox[...][:, 0, :])

    @pl.when(far)
    def _():
        first(block, n_dp, block_recv).wait()
        take(block[...][:, 0, :])
        send_t1()

    def pair(turned, k):
        return jnp.concatenate([turned[k : k + 1], turned[16 + k : 17 + k]], axis=0)

    turned = jnp.transpose(quiet[...])
    t2_src[...] = pair(turned, 0)
    t2[pl.ds(tp, 1)] = t2_src[...][None]

    @pl.when(skips)
    def _():
        for peer in tp_peers:

            @pl.when(peer != first_tp)
            def _():
                send_one(t2_src, t2, t2_send, t2_recv, peer)

    @pl.when(jnp.logical_not(skips))
    def _():
        for peer in tp_peers:
            send_one(t2_src, t2, t2_send, t2_recv, peer)


    forward = pltpu.make_async_remote_copy(
        src_ref=relay,
        dst_ref=block,
        send_sem=relay_send,
        recv_sem=block_recv,
        device_id={"dp": partner},
        device_id_type=MESH,
    )

    @pl.when(near)
    def _():
        pl.semaphore_wait(line_in, n_tp - 1)
        relay[...] = inbox[...][:, 1:2, :]
        forward.start()

    ref_rows, held_returns = pair(turned, 2), pair(turned, 4)
    same = (turned[12:13] == pid).astype(F32)
    count = jnp.sum(same * turned[6:7], axis=1, keepdims=True)
    summed = jnp.sum(same * turned[8:9], axis=1, keepdims=True)
    square = jnp.sum(same * turned[10:11], axis=1, keepdims=True)
    floor = jnp.maximum(count, 1.0)
    mean = summed / floor
    var = (square - mean * summed) / floor
    whitened = (advantages - mean) * lax.rsqrt(var + 1.0)

    first(t1, n_tp - 1, t1_recv).wait()
    shards = t1[...]
    values = jnp.sum(shards[:, 6:8], axis=0)
    w_wide = jnp.pad(w_row.astype(F32), ((0, 0), (0, -feats % 128)))
    w_all = jnp.transpose(jnp.broadcast_to(w_wide, (128, w_wide.shape[1])))[:feats]
    coeff = jnp.where(held_returns > 1e29, 0.0, 32.0 * (values - held_returns))
    for j in range(2):
        grad_out[j] = (w_all * coeff[j : j + 1]).astype(jnp.bfloat16)

    tops = shards[:, 0:2]
    row_max = jnp.max(tops, axis=0)
    total = jnp.sum(shards[:, 2:4] * jnp.exp(tops - row_max[None]), axis=0)
    target = jnp.sum(shards[:, 4:6], axis=0)
    logprob = target - (row_max + jnp.log(total))
    ratio = jnp.exp(jnp.clip(logprob - old_v[...], -20.0, 20.0))
    surrogate = jnp.maximum(-whitened * ratio, -whitened * jnp.clip(ratio, 0.8, 1.2))
    surrogate = jnp.where(whitened < 0.0, jnp.minimum(surrogate, -3.0 * whitened), surrogate)
    drift = jnp.clip(ref_rows - logprob, -20.0, 20.0)
    penalty = jnp.clip(jnp.exp(drift) - drift - 1.0, -10.0, 10.0)
    policy = live * (surrogate + 0.1 * penalty)
    scale = 0.25 * live

    @pl.when(is_first)
    def _():
        first(t2, n_tp - 1 - len(sources), t2_recv).wait()
        pltpu.make_async_copy(direct, direct, direct_recv).wait()
        take(jnp.sum(direct[...], axis=0)[:, 0, :])
        t2[0] = pair(jnp.transpose(quiet[...]), 0)
        for column in sources[1:]:
            t2[column] = jnp.zeros((2, 128), F32)

    @pl.when(jnp.logical_not(is_first))
    def _():
        first(t2, n_tp - 1, t2_recv).wait()

    error = jnp.sum(t2[...], axis=0) - returns
    loss_out[...] = policy + scale * error * error

    first(t1, n_tp - 1, t1_send).wait()

    @pl.when(skips)
    def _():
        first(t2, n_tp - 2, t2_send).wait()

    @pl.when(jnp.logical_not(skips))
    def _():
        first(t2, n_tp - 1, t2_send).wait()

    @pl.when(straight)
    def _():
        first(msg, 1, direct_send).wait()

    @pl.when(near)
    def _():
        first(msg, n_dp // 2 - 1, dp_send).wait()
        first(relay, n_dp, relay_send).wait()

    @pl.when(far)
    def _():
        first(msg, n_dp // 2, dp_send).wait()


def finish(loss, grad, loss_out, grad_out, sems):
    copies = [
        pltpu.make_async_copy(src, dst, sems.at[n])
        for n, (src, dst) in enumerate([(grad, grad_out), (loss, loss_out)])
    ]
    for copy in copies:
        copy.start()
    for copy in copies:
        copy.wait()


def per_device(sizes, *arrays):
    (
        logits, ids, mask, lengths, prompt_of, old, ref, adv, ret, critic, weight
    ) = arrays
    seqs, length, vocab = logits.shape
    batch, tile, feats = critic.shape
    xs, zs, ys = sizes
    any_ref, vmem = pl.BlockSpec(memory_space=pl.ANY), pl.BlockSpec(memory_space=pltpu.VMEM)
    dma = pltpu.SemaphoreType.DMA
    vm = pltpu.VMEM
    loss, grad = pl.pallas_call(
        functools.partial(kernel, xs, zs, ys, vocab),
        out_shape=(
            vm((seqs, length), F32),
            vm((tile, feats, batch), jnp.bfloat16),
        ),
        in_specs=[any_ref] * 11,
        out_specs=[vmem] * 2,
        scratch_shapes=[
            vm(logits.shape, jnp.bfloat16),
            vm((tile, feats, batch), jnp.bfloat16),
            vm((seqs, length), jnp.int32),
            vm((seqs, length), jnp.int32),
            vm((seqs, length), F32),
            vm((tile, batch), jnp.bfloat16),
            vm((seqs, length), F32),
            vm((seqs, length), F32),
            vm((feats,), jnp.bfloat16),
            pltpu.SMEM((seqs,), jnp.int32),
            pltpu.SMEM((seqs,), jnp.int32),
            vm((128, 128), F32),
            vm((32, 2, 128), F32),
            vm((64, 2, 128), F32),
            vm((64, 1, 128), F32),
            vm((64, 1, 128), F32),
            vm((9, 64, 2, 128), F32),
            vm((128, 128), F32),
            vm((128, 8), jnp.int32),
            vm((128, 128), F32),
            vm((8, 128), F32),
            vm((2 * ys, 8, 128), F32),
            vm((seqs, length), F32),
            vm((2 * ys, seqs, length), F32),
            dma((4,)), dma((13,)), dma, dma, dma, dma, dma, dma,
            dma, dma, dma, dma, pltpu.SemaphoreType.REGULAR, pltpu.SemaphoreType.REGULAR,
        ],
        compiler_params=pltpu.CompilerParams(collective_id=0, has_side_effects=True),
        name="ppo_all",
    )(
        logits, ids, mask, lengths, prompt_of, old, ref.T, adv, ret,
        jnp.transpose(critic, (1, 2, 0)), weight,
    )
    loss, grad = pl.pallas_call(
        finish,
        out_shape=(
            jax.ShapeDtypeStruct((seqs, length), F32),
            jax.ShapeDtypeStruct((tile, feats, batch), jnp.bfloat16),
        ),
        in_specs=[vmem] * 2,
        out_specs=[any_ref] * 2,
        scratch_shapes=[dma((2,))],
        compiler_params=pltpu.CompilerParams(vmem_limit_bytes=2**20),
        name="ppo_finish",
    )(loss, grad)
    return loss, jnp.transpose(grad, (2, 0, 1))


def solution(mesh):
    in_specs = (
        P("dp", None, "tensor"),
        P("dp", None),
        P("dp", None),
        P("dp"),
        P("dp"),
        P("dp", None),
        P(None, "dp"),
        P("dp", None),
        P("dp", None),
        P(None, "dp", "tensor"),
        P("tensor"),
    )
    out_specs = (P("dp", None), P(None, "dp", "tensor"))
    dp_size, tp_size = mesh.shape["dp"], mesh.shape["tensor"]
    sizes = (4, dp_size // 4, tp_size // 2)
    return jax.shard_map(
        functools.partial(per_device, sizes),
        mesh=mesh,
        in_specs=in_specs,
        out_specs=out_specs,
        check_vma=False,
    )
```
